32 devices in a mesh: tp: 4 (over z), dp: 8 (over y, x, core).
Axes of the slice: x: 2, y: 2, z: 4, core: 2. Of those that a mesh axis runs over, the one named last changes fastest.
Arguments:
- hidden: bfloat16 [2048, 640], P('dp')
- embedding: bfloat16 [262144, 640], P('tp')
- norm_weight: float32 [640], replicated
- teach_ids: int32 [2048, 256], P('dp')
- teach_prob: float32 [2048, 256], P('dp')
- tok_mask: float32 [2048], P('dp')
Outputs:
- output 1: float32 [], replicated
- output 2: bfloat16 [2048, 640], P('dp')
- output 3: float32 [262144, 640], P('tp', 'dp')
- output 4: float32 [640], replicated
All inputs are finite; a program needn't handle non-finite values.
Results may differ from the reference program's by a relative error of at most 0.001.
Values sent between devices are 32-bit elements.
A program may use at most 1 GiB of HBM per device.

```python
import jax
import jax.numpy as jnp
from jax import lax

MODEL_DIM = 640
VOCAB_SIZE = 262144
TEACH_TOP = 256
NUM_TOKENS = 2048

EPS_NORM = 1e-6
LOGIT_GAIN = 2.5
HALF_TOP = TEACH_TOP // 2
FREQ_VOCAB = VOCAB_SIZE // 8
ROW_BLOCK = min(NUM_TOKENS, 64)


def draw_teacher_ids(key_ids):
    key_low, key_high, key_perm = jax.random.split(key_ids, 3)
    low_band = FREQ_VOCAB // HALF_TOP
    high_band = (VOCAB_SIZE - FREQ_VOCAB) // HALF_TOP
    slot_pos = jnp.arange(HALF_TOP, dtype=jnp.int32)
    high_width = jnp.where(slot_pos == HALF_TOP - 1, VOCAB_SIZE - FREQ_VOCAB - (HALF_TOP - 1) * high_band, high_band)
    low_off = jax.random.randint(key_low, (NUM_TOKENS, HALF_TOP), 0, low_band, dtype=jnp.int32)
    high_raw = jax.random.randint(key_high, (NUM_TOKENS, HALF_TOP), 0, 1 << 24, dtype=jnp.int32)
    high_off = high_raw % high_width[None, :]
    low_off = low_off.at[0, 0].set(0)
    high_off = high_off.at[0, HALF_TOP - 1].set(high_width[HALF_TOP - 1] - 1)
    low_ids = slot_pos[None, :] * low_band + low_off
    high_ids = FREQ_VOCAB + slot_pos[None, :] * high_band + high_off
    all_ids = jnp.concatenate([low_ids, high_ids], axis=1)
    row_keys = jax.random.split(key_perm, NUM_TOKENS)
    perm_rows = jax.vmap(lambda row_key: jax.random.permutation(row_key, TEACH_TOP))(row_keys)
    return jnp.take_along_axis(all_ids, perm_rows.astype(jnp.int32), axis=1)


def draw_mask(key_mask):
    keep_flag = jax.random.randint(key_mask, (NUM_TOKENS,), 0, 8, dtype=jnp.int32) != 0
    return keep_flag.astype(jnp.float32).at[0].set(1.0)


def setup_inputs(seed: int = 0) -> dict:
    root_key = jax.random.key(seed)
    key_h, key_e, key_w, key_ids, key_prob, key_mask = jax.random.split(root_key, 6)
    hidden = jax.random.normal(key_h, (NUM_TOKENS, MODEL_DIM), jnp.float32).astype(jnp.bfloat16)
    embed_scale = LOGIT_GAIN * MODEL_DIM ** -0.5
    embedding = (jax.random.normal(key_e, (VOCAB_SIZE, MODEL_DIM), jnp.float32) * embed_scale).astype(jnp.bfloat16)
    norm_weight = 0.5 * jax.random.normal(key_w, (MODEL_DIM,), jnp.float32)
    teach_ids = draw_teacher_ids(key_ids)
    teach_prob = jax.nn.softmax(jax.random.normal(key_prob, (NUM_TOKENS, TEACH_TOP), jnp.float32), axis=1)
    tok_mask = draw_mask(key_mask)
    return {'hidden': hidden, 'embedding': embedding, 'norm_weight': norm_weight, 'teach_ids': teach_ids, 'teach_prob': teach_prob, 'tok_mask': tok_mask}


def reference(hidden, embedding, norm_weight, teach_ids, teach_prob, tok_mask):
    mask_total = jnp.sum(tok_mask)
    scale_w = 1.0 + norm_weight
    num_blocks = NUM_TOKENS // ROW_BLOCK
    row_ids = jnp.arange(ROW_BLOCK)[:, None]

    def block_step(acc_embed, block_in):
        h_blk, ids_blk, prob_blk, mask_blk = block_in
        h_f32 = h_blk.astype(jnp.float32)
        inv_rms = lax.rsqrt(jnp.mean(h_f32 * h_f32, axis=1, keepdims=True) + EPS_NORM)
        normed = h_f32 * inv_rms
        normed_bf = (normed * scale_w).astype(jnp.bfloat16)
        logits = lax.dot_general(normed_bf, embedding, (((1,), (1,)), ((), ())), preferred_element_type=jnp.float32)
        row_max = jnp.max(logits, axis=1, keepdims=True)
        log_norm = row_max + jnp.log(jnp.sum(jnp.exp(logits - row_max), axis=1, keepdims=True))
        picked = jnp.take_along_axis(logits, ids_blk, axis=1)
        teach_sum = jnp.sum(prob_blk * picked, axis=1)
        loss_part = jnp.sum(mask_blk * (teach_sum - log_norm[:, 0]))
        weight = (mask_blk / mask_total)[:, None]
        soft_prob = jnp.exp(logits - log_norm)
        d_logits = (soft_prob * weight).at[row_ids, ids_blk].add(-prob_blk * weight)
        dlogit_bf = d_logits.astype(jnp.bfloat16)
        grad_u = jnp.dot(dlogit_bf, embedding, preferred_element_type=jnp.float32)
        acc_embed = acc_embed + lax.dot_general(dlogit_bf, normed_bf, (((0,), (0,)), ((), ())), preferred_element_type=jnp.float32)
        d_normed = grad_u * scale_w
        grad_h = inv_rms * (d_normed - normed * jnp.mean(d_normed * normed, axis=1, keepdims=True))
        grad_w = jnp.sum(grad_u * normed, axis=0)
        return acc_embed, (loss_part, grad_h.astype(jnp.bfloat16), grad_w)

    blocks = (hidden.reshape(num_blocks, ROW_BLOCK, MODEL_DIM), teach_ids.reshape(num_blocks, ROW_BLOCK, TEACH_TOP), teach_prob.reshape(num_blocks, ROW_BLOCK, TEACH_TOP), tok_mask.reshape(num_blocks, ROW_BLOCK))
    acc_init = jnp.zeros((VOCAB_SIZE, MODEL_DIM), jnp.float32)
    grad_embed, (loss_parts, grad_hidden, norm_parts) = lax.scan(block_step, acc_init, blocks)
    loss_mean = -jnp.sum(loss_parts) / mask_total
    return loss_mean, grad_hidden.reshape(NUM_TOKENS, MODEL_DIM), grad_embed, jnp.sum(norm_parts, axis=0)
```

```python
import functools

import jax
import jax.numpy as jnp
from jax import lax
from jax.experimental import pallas as pl
from jax.experimental.pallas import tpu as pltpu
from jax.sharding import PartitionSpec as P

EPS_NORM = 1e-6
LANES = 256
MIB = 1024 * 1024
NT = (((1,), (1,)), ((), ()))


def stats_kernel(emb_ref, ut_ref, max_ref, sum_ref, *, sub):
    @pl.when(pl.program_id(0) == 0)
    def _():
        max_ref[...] = jnp.full(max_ref.shape, -jnp.inf, jnp.float32)
        sum_ref[...] = jnp.zeros(sum_ref.shape, jnp.float32)

    rows = emb_ref.shape[0]
    toks = ut_ref.shape[1]
    for c in range(rows // sub):
        z = jnp.dot(emb_ref[c * sub:(c + 1) * sub, :], ut_ref[...], preferred_element_type=jnp.float32)
        z = z.reshape(sub // 8, 8, toks)
        old = max_ref[...]
        new = jnp.maximum(old, jnp.max(z, axis=0))
        sum_ref[...] = sum_ref[...] * jnp.exp(old - new) + jnp.sum(jnp.exp(z - new[None]), axis=0)
        max_ref[...] = new


def local_stats(emb, ut, rows=2048, sub=512):
    vocab, dim = emb.shape
    toks = ut.shape[1]
    shape = jax.ShapeDtypeStruct((8, toks), jnp.float32)
    return pl.pallas_call(
        functools.partial(stats_kernel, sub=sub),
        grid=(vocab // rows,),
        in_specs=[pl.BlockSpec((rows, dim), lambda i: (i, 0)), pl.BlockSpec((dim, toks), lambda i: (0, 0))],
        out_specs=[pl.BlockSpec((8, toks), lambda i: (0, 0))] * 2,
        out_shape=[shape, shape],
        compiler_params=pltpu.CompilerParams(vmem_limit_bytes=40 * MIB),
        cost_estimate=pl.CostEstimate(flops=2 * vocab * dim * toks, bytes_accessed=2 * vocab * dim, transcendentals=vocab * toks),
    )(emb, ut)


def teacher_kernel(base_ref, ids_ref, prob_ref, out_ref, *, high, group):
    top = ids_ref.shape[1]
    base = base_ref[0]
    high_iota = lax.broadcasted_iota(jnp.int32, (high, top), 0)
    low_iota = lax.broadcasted_iota(jnp.int32, (LANES, top), 0)

    def step(i, _):
        rows = pl.ds(pl.multiple_of(i * group, group), group)
        local = ids_ref[rows, :] - base
        hi = local >> 8
        lo = local & (LANES - 1)
        prob = prob_ref[rows, :]
        p1 = prob.astype(jnp.bfloat16).astype(jnp.float32)
        r1 = prob - p1
        p2 = r1.astype(jnp.bfloat16).astype(jnp.float32)
        p3 = r1 - p2
        parts = []
        for j in range(group):
            hit = high_iota == jnp.broadcast_to(hi[j:j + 1, :], (high, top))
            left = [jnp.where(hit, jnp.broadcast_to(p[j:j + 1, :], (high, top)), 0.0).astype(jnp.bfloat16) for p in (p1, p2, p3)]
            right = jnp.where(low_iota == jnp.broadcast_to(lo[j:j + 1, :], (LANES, top)), 1.0, 0.0).astype(jnp.bfloat16)
            dense = lax.dot_general(jnp.concatenate(left, axis=0), right, NT, preferred_element_type=jnp.float32)
            parts.append(dense[:high] + (dense[high:2 * high] + dense[2 * high:]))
        out_ref[:, rows, :] = jnp.swapaxes(jnp.stack(parts, axis=0), 0, 1)
        return 0

    lax.fori_loop(0, ids_ref.shape[0] // group, step, 0)


def teacher_dense(base, ids, prob, high, block=128):
    toks, top = ids.shape
    return pl.pallas_call(
        functools.partial(teacher_kernel, high=high, group=8),
        grid=(toks // block,),
        in_specs=[pl.BlockSpec(memory_space=pltpu.SMEM), pl.BlockSpec((block, top), lambda i: (i, 0)), pl.BlockSpec((block, top), lambda i: (i, 0))],
        out_specs=pl.BlockSpec((high, block, LANES), lambda i: (0, i, 0)),
        out_shape=jax.ShapeDtypeStruct((high, toks, LANES), jnp.float32),
        compiler_params=pltpu.CompilerParams(vmem_limit_bytes=40 * MIB),
        cost_estimate=pl.CostEstimate(flops=6 * high * LANES * toks * top, bytes_accessed=4 * high * LANES * toks, transcendentals=0),
    )(base, ids, prob)


def main_kernel(emb, dense, u_ref, ut_ref, logz_ref, w_ref, out, du_ref, tsum_ref,
                emb_buf, dense_buf, g_buf, de_buf, in_sem, send_sem, recv_sem, own_sem, *, tile, chunk, peers):
    toks, dim = u_ref.shape
    cols = dim // peers
    tp = lax.axis_index('tp')
    me = lax.axis_index('dp')
    block = emb.shape[0] // peers
    tiles = block // tile
    per = tile // LANES

    barrier = pltpu.get_barrier_semaphore()
    for s in range(1, peers):
        pl.semaphore_signal(barrier, inc=1, device_id=(tp, me ^ s), device_id_type=pl.DeviceIdType.MESH)
    pl.semaphore_wait(barrier, peers - 1)

    def fetch(t, slot):
        rows = pl.ds(pl.multiple_of(me * block + t * tile, tile), tile)
        return (
            pltpu.make_async_copy(emb.at[rows, :], emb_buf.at[slot], in_sem.at[slot, 0]),
            pltpu.make_async_copy(dense.at[pl.ds(t * per, per)], dense_buf.at[slot], in_sem.at[slot, 1]),
        )

    def send(t, s):
        to = me ^ s
        return pltpu.make_async_remote_copy(
            src_ref=de_buf.at[t, pl.ds(pl.multiple_of(to * cols, 8), cols), :],
            dst_ref=out.at[:, pl.ds(pl.multiple_of(me * block + t * tile, tile), tile)],
            send_sem=send_sem.at[t, s],
            recv_sem=recv_sem.at[t, s],
            device_id=(tp, to),
            device_id_type=pl.DeviceIdType.MESH,
        )

    def keep(t):
        return pltpu.make_async_copy(
            de_buf.at[t, pl.ds(pl.multiple_of(me * cols, 8), cols), :],
            out.at[:, pl.ds(pl.multiple_of(me * block + t * tile, tile), tile)],
            own_sem.at[t],
        )

    for c in fetch(0, 0):
        c.start()
    du_ref[...] = jnp.zeros(du_ref.shape, jnp.float32)
    tsum_ref[...] = jnp.zeros(tsum_ref.shape, jnp.float32)

    def step(t, _):
        slot = lax.rem(t, 2)
        for c in fetch(t, slot):
            c.wait()

        @pl.when(t + 1 < tiles)
        def _():
            for c in fetch(t + 1, 1 - slot):
                c.start()

        e = emb_buf[slot]

        def part(i, acc):
            rows = pl.ds(pl.multiple_of(i * chunk, chunk), chunk)
            z = lax.dot_general(u_ref[rows, :], e, NT, preferred_element_type=jnp.float32)
            w = w_ref[rows, :]
            logz = logz_ref[rows, :]
            for h in range(per):
                zh = z[:, h * LANES:(h + 1) * LANES]
                q = dense_buf[slot, h, rows, :] * w
                g_buf[rows, h * LANES:(h + 1) * LANES] = (jnp.exp(zh - logz) * w - q).astype(jnp.bfloat16)
                acc = acc + jnp.sum((q * zh).reshape(chunk // 8, 8, LANES), axis=0)
            du_ref[rows, :] += jnp.dot(g_buf[rows, :], e, preferred_element_type=jnp.float32)
            return acc

        tsum_ref[...] = lax.fori_loop(0, toks // chunk, part, tsum_ref[...])
        de_buf[t] = jnp.dot(ut_ref[...], g_buf[...], preferred_element_type=jnp.float32)
        keep(t).start()
        for s in range(1, peers):
            send(t, s).start()
        return 0

    lax.fori_loop(0, tiles, step, 0)

    def drain(t, _):
        keep(t).wait()
        for s in range(1, peers):
            send(t, s).wait()
        return 0

    lax.fori_loop(0, tiles, drain, 0)


def main_pass(emb, dense, u, ut, logz, w, peers, tile=512, chunk=512):
    vocab, dim = emb.shape
    toks = u.shape[0]
    block = vocab // peers
    tiles = block // tile
    per = tile // LANES
    vmem = pl.BlockSpec(memory_space=pltpu.VMEM)
    hbm = pl.BlockSpec(memory_space=pl.ANY)
    return pl.pallas_call(
        functools.partial(main_kernel, tile=tile, chunk=chunk, peers=peers),
        in_specs=[hbm, hbm, vmem, vmem, vmem, vmem],
        out_specs=[hbm, vmem, vmem],
        out_shape=[
            jax.ShapeDtypeStruct((dim // peers, vocab), jnp.float32),
            jax.ShapeDtypeStruct((toks, dim), jnp.float32),
            jax.ShapeDtypeStruct((8, LANES), jnp.float32),
        ],
        scratch_shapes=[
            pltpu.VMEM((2, tile, dim), jnp.bfloat16),
            pltpu.VMEM((2, per, toks, LANES), jnp.float32),
            pltpu.VMEM((toks, tile), jnp.bfloat16),
            pltpu.VMEM((tiles, dim, tile), jnp.float32),
            pltpu.SemaphoreType.DMA((2, 2)),
            pltpu.SemaphoreType.DMA((tiles, peers)),
            pltpu.SemaphoreType.DMA((tiles, peers)),
            pltpu.SemaphoreType.DMA((tiles,)),
        ],
        compiler_params=pltpu.CompilerParams(vmem_limit_bytes=63 * MIB, collective_id=0, has_side_effects=True),
        cost_estimate=pl.CostEstimate(flops=6 * block * dim * toks, bytes_accessed=4 * block * toks, transcendentals=block * toks),
    )(emb, dense, u, ut, logz, w)


def solution(mesh):
    peers = mesh.shape['dp']

    def local_head(hidden, embedding, norm_weight, teach_ids, teach_prob, tok_mask):
        vocab_local = embedding.shape[0]
        toks = hidden.shape[0]
        block = vocab_local // peers
        high = block // LANES
        dim = hidden.shape[1]
        tp = lax.axis_index('tp')
        dp = lax.axis_index('dp')
        scale_w = 1.0 + norm_weight
        h_f32 = hidden.astype(jnp.float32)
        inv_rms = lax.rsqrt(jnp.mean(h_f32 * h_f32, axis=1, keepdims=True) + EPS_NORM)
        normed = h_f32 * inv_rms

        ids_all = lax.all_gather(teach_ids, 'dp', axis=0, tiled=True)
        prob_all = lax.all_gather(teach_prob, 'dp', axis=0, tiled=True)
        normed_all = lax.all_gather(normed, 'dp', axis=0, tiled=True)

        u_loc = (normed * scale_w).astype(jnp.bfloat16)
        part_max, part_sum = local_stats(embedding, u_loc.T)
        loc_max = jnp.max(part_max, axis=0)
        loc_sum = jnp.sum(part_sum * jnp.exp(part_max - loc_max), axis=0)
        stats = lax.all_gather(jnp.stack([loc_max, loc_sum, tok_mask]), ('tp', 'dp'), axis=0, tiled=False)
        stats = stats.reshape(-1, peers, 3, toks)
        row_max = jnp.max(stats[:, :, 0], axis=0)
        sum_exp = jnp.sum(stats[:, :, 1] * jnp.exp(stats[:, :, 0] - row_max), axis=0)
        log_norm = (row_max + jnp.log(sum_exp)).reshape(-1, 1)
        mask = stats[0, :, 2].reshape(-1, 1)
        weight = mask / jnp.sum(mask)

        base = (tp * vocab_local + dp * block).astype(jnp.int32).reshape(1)
        dense = teacher_dense(base, ids_all, prob_all, high)
        u_all = (normed_all * scale_w).astype(jnp.bfloat16)
        de_t, du_part, tsum = main_pass(embedding, dense, u_all, u_all.T, log_norm, weight, peers)

        du_loc = lax.psum_scatter(du_part, 'dp', scatter_dimension=0, tiled=True)
        sums = jnp.concatenate([jnp.sum(du_loc * normed, axis=0), jnp.sum(tsum, axis=0)[:128], jnp.sum(tsum, axis=0)[128:]])
        sums = lax.psum(sums, ('tp', 'dp'))
        grad_norm = sums[:dim]
        loss_mean = jnp.sum(weight * log_norm) - jnp.sum(sums[dim:])
        grad_u = lax.psum(du_loc, 'tp')
        d_normed = grad_u * scale_w
        grad_hidden = (inv_rms * (d_normed - normed * jnp.mean(d_normed * normed, axis=1, keepdims=True))).astype(jnp.bfloat16)
        return loss_mean, grad_hidden, de_t.T, grad_norm

    return jax.shard_map(local_head, mesh=mesh, in_specs=(P('dp', None), P('tp', None), P(None), P('dp', None), P('dp', None), P('dp')), out_specs=(P(), P('dp', None), P('tp', 'dp'), P(None)), check_vma=False)
```

```python
import functools

import jax
import jax.numpy as jnp
from jax import lax
from jax.experimental import pallas as pl
from jax.experimental.pallas import tpu as pltpu
from jax.sharding import PartitionSpec as P

EPS_NORM = 1e-6
LANES = 128
MIB = 1024 * 1024
NT = (((1,), (1,)), ((), ()))
MESH = pl.DeviceIdType.MESH


def swap_all(src, dst, send_sem, recv_sem, groups, peers):
    total = groups * peers
    me = lax.axis_index('tp') * peers + lax.axis_index('dp')

    def copy(s):
        to = lax.rem(me + s, total)
        return pltpu.make_async_remote_copy(
            src_ref=src, dst_ref=dst.at[me], send_sem=send_sem.at[s], recv_sem=recv_sem.at[s],
            device_id=(to // peers, lax.rem(to, peers)), device_id_type=MESH)

    def start(s, _):
        copy(s).start()
        return 0

    def wait(s, _):
        copy(s).wait()
        return 0

    return (lambda: lax.fori_loop(1, total, start, 0)), (lambda: lax.fori_loop(1, total, wait, 0))


def enter_all(groups, peers):
    total = groups * peers
    me = lax.axis_index('tp') * peers + lax.axis_index('dp')
    barrier = pltpu.get_barrier_semaphore()

    def greet(s, _):
        to = lax.rem(me + s, total)
        pl.semaphore_signal(barrier, inc=1, device_id=(to // peers, lax.rem(to, peers)), device_id_type=MESH)
        return 0

    lax.fori_loop(1, total, greet, 0)
    pl.semaphore_wait(barrier, total - 1)


def stats_kernel(emb_ref, ut_ref, mask_ref, out_ref, max_ref, sum_ref, mine_ref, all_ref, send_sem, recv_sem, *, sub, groups, peers):
    @pl.when(pl.program_id(0) == 0)
    def _():
        max_ref[...] = jnp.full(max_ref.shape, -jnp.inf, jnp.float32)
        sum_ref[...] = jnp.zeros(sum_ref.shape, jnp.float32)

    rows = emb_ref.shape[0]
    toks = ut_ref.shape[1]
    for c in range(rows // sub):
        z = jnp.dot(emb_ref[c * sub:(c + 1) * sub, :], ut_ref[...], preferred_element_type=jnp.float32)
        z = z.reshape(sub // 8, 8, toks)
        old = max_ref[...]
        new = jnp.maximum(old, jnp.max(z, axis=0))
        sum_ref[...] = sum_ref[...] * jnp.exp(old - new) + jnp.sum(jnp.exp(z - new[None]), axis=0)
        max_ref[...] = new

    @pl.when(pl.program_id(0) == pl.num_programs(0) - 1)
    def _():
        top = jnp.max(max_ref[...], axis=0, keepdims=True)
        tot = jnp.sum(sum_ref[...] * jnp.exp(max_ref[...] - top), axis=0, keepdims=True)
        row = lax.broadcasted_iota(jnp.int32, (8, toks), 0)
        mine = jnp.where(row == 0, top, jnp.where(row == 1, tot, mask_ref[...]))
        mine_ref[...] = mine
        me = lax.axis_index('tp') * peers + lax.axis_index('dp')
        all_ref[me] = mine
        enter_all(groups, peers)
        start, wait = swap_all(mine_ref, all_ref, send_sem, recv_sem, groups, peers)
        start()
        wait()
        out_ref[...] = all_ref[...]


def local_stats(emb, ut, mask, groups, peers, rows=2048, sub=512):
    vocab, dim = emb.shape
    toks = ut.shape[1]
    total = groups * peers
    return pl.pallas_call(
        functools.partial(stats_kernel, sub=sub, groups=groups, peers=peers),
        grid=(vocab // rows,),
        in_specs=[pl.BlockSpec((rows, dim), lambda i: (i, 0)), pl.BlockSpec((dim, toks), lambda i: (0, 0)), pl.BlockSpec((1, toks), lambda i: (0, 0))],
        out_specs=pl.BlockSpec((total, 8, toks), lambda i: (0, 0, 0)),
        out_shape=jax.ShapeDtypeStruct((total, 8, toks), jnp.float32),
        scratch_shapes=[pltpu.VMEM((8, toks), jnp.float32)] * 3 + [pltpu.VMEM((total, 8, toks), jnp.float32)] + [pltpu.SemaphoreType.DMA((total,))] * 2,
        compiler_params=pltpu.CompilerParams(vmem_limit_bytes=40 * MIB, collective_id=1, has_side_effects=True),
        cost_estimate=pl.CostEstimate(flops=2 * vocab * dim * toks, bytes_accessed=2 * vocab * dim, transcendentals=vocab * toks),
    )(emb, ut, mask)


def teacher_kernel(base_ref, ids_ref, prob_ref, out_ref, *, high, group):
    top = ids_ref.shape[1]
    base = base_ref[0]
    bf16 = jnp.bfloat16
    high_iota = lax.broadcasted_iota(jnp.int32, (high, top), 0).astype(jnp.float32).astype(bf16)
    low_iota = lax.broadcasted_iota(jnp.int32, (LANES, top), 0).astype(jnp.float32).astype(bf16)

    def spread(row, n):
        row = jnp.broadcast_to(row, (16, top)).astype(bf16)
        return jnp.broadcast_to(row[None], (n // 16, 16, top)).reshape(n, top)

    def step(i, _):
        rows = pl.ds(pl.multiple_of(i * group, group), group)
        local = ids_ref[rows, :] - base
        hi = local >> (LANES.bit_length() - 1)
        lo = (local & (LANES - 1)).astype(jnp.float32)
        hi = jnp.where((local >= 0) & (hi < high), hi, -1).astype(jnp.float32)
        prob = prob_ref[rows, :]
        p1 = prob.astype(bf16).astype(jnp.float32)
        r1 = prob - p1
        p2 = r1.astype(bf16).astype(jnp.float32)
        p3 = r1 - p2
        parts = []
        for j in range(group):
            hit = high_iota == spread(hi[j:j + 1, :], high)
            left = [jnp.where(hit, spread(p[j:j + 1, :], high), jnp.zeros((), bf16)) for p in (p1, p2, p3)]
            right = jnp.where(low_iota == spread(lo[j:j + 1, :], LANES), jnp.ones((), bf16), jnp.zeros((), bf16))
            dense = lax.dot_general(jnp.concatenate(left, axis=0), right, NT, preferred_element_type=jnp.float32)
            parts.append(dense[:high] + (dense[high:2 * high] + dense[2 * high:]))
        out_ref[:, rows, :] = jnp.swapaxes(jnp.stack(parts, axis=0), 0, 1)
        return 0

    lax.fori_loop(0, ids_ref.shape[0] // group, step, 0)


def teacher_dense(base, ids, prob, high, block=128):
    toks, top = ids.shape
    return pl.pallas_call(
        functools.partial(teacher_kernel, high=high, group=16),
        grid=(toks // block,),
        in_specs=[pl.BlockSpec(memory_space=pltpu.SMEM), pl.BlockSpec((block, top), lambda i: (i, 0)), pl.BlockSpec((block, top), lambda i: (i, 0))],
        out_specs=pl.BlockSpec((high, block, LANES), lambda i: (0, i, 0)),
        out_shape=jax.ShapeDtypeStruct((high, toks, LANES), jnp.float32),
        compiler_params=pltpu.CompilerParams(vmem_limit_bytes=40 * MIB),
        cost_estimate=pl.CostEstimate(flops=6 * high * LANES * toks * top, bytes_accessed=4 * high * LANES * toks, transcendentals=0),
    )(base, ids, prob)


def main_kernel(emb, dense, u_ref, ut_ref, logz_ref, w_ref, y_ref, out, du_full, sums_out,
                emb_buf, dense_buf, g_buf, de_buf, du_ref, tsum_ref, core_buf, z_buf, xy_buf, tot_ref, mine_ref, du_out, sums_ref,
                in_sem, send_sem, recv_sem, own_sem, red_send, red_recv, all_send, all_recv,
                *, tile, chunk, held, groups, peers):
    toks, dim = u_ref.shape
    cols = dim // peers
    local = toks // peers
    part_rows = local // groups
    tp = lax.axis_index('tp')
    me = lax.axis_index('dp')
    block = emb.shape[0] // peers
    tiles = block // tile
    per = tile // LANES
    pairs = peers // 2
    core = lax.rem(me, 2)
    chip = me // 2

    enter_all(groups, peers)

    def fetch(t, slot):
        rows = pl.ds(pl.multiple_of(me * block + t * tile, tile), tile)
        return (
            pltpu.make_async_copy(emb.at[rows, :], emb_buf.at[slot], in_sem.at[slot, 0]),
            pltpu.make_async_copy(dense.at[pl.ds(t * per, per)], dense_buf.at[slot], in_sem.at[slot, 1]),
        )

    def send(t, s):
        to = me ^ s
        return pltpu.make_async_remote_copy(
            src_ref=de_buf.at[t, pl.ds(pl.multiple_of(to * cols, 8), cols), :],
            dst_ref=out.at[:, pl.ds(pl.multiple_of(me * block + t * tile, tile), tile)],
            send_sem=send_sem.at[t, s],
            recv_sem=recv_sem.at[t, s],
            device_id=(tp, to),
            device_id_type=MESH,
        )

    def keep(t):
        return pltpu.make_async_copy(
            de_buf.at[t, pl.ds(pl.multiple_of(me * cols, 8), cols), :],
            out.at[:, pl.ds(pl.multiple_of(me * block + t * tile, tile), tile)],
            own_sem.at[t],
        )

    def send_tile(t):
        for s in range(peers - 1, 0, -1):
            send(t, s).start()

    for c in fetch(0, 0):
        c.start()
    du_ref[...] = jnp.zeros(du_ref.shape, jnp.float32)
    tsum_ref[...] = jnp.zeros(tsum_ref.shape, jnp.float32)

    def step(t, _):
        slot = lax.rem(t, 2)
        for c in fetch(t, slot):
            c.wait()

        @pl.when(t + 1 < tiles)
        def _():
            for c in fetch(t + 1, 1 - slot):
                c.start()

        e = emb_buf[slot]

        def part(i, acc):
            rows = pl.ds(pl.multiple_of(i * chunk, chunk), chunk)
            z = lax.dot_general(u_ref[rows, :], e, NT, preferred_element_type=jnp.float32)
            w = w_ref[rows, :]
            logz = logz_ref[rows, :]
            for h in range(per):
                zh = z[:, h * LANES:(h + 1) * LANES]
                q = dense_buf[slot, h, rows, :] * w
                g_buf[rows, h * LANES:(h + 1) * LANES] = (jnp.exp(zh - logz) * w - q).astype(jnp.bfloat16)
                acc = acc + jnp.sum((q * zh).reshape(chunk // 8, 8, LANES), axis=0)
            du_ref[rows, :] += jnp.dot(g_buf[rows, :], e, preferred_element_type=jnp.float32)
            return acc

        tsum_ref[...] = lax.fori_loop(0, toks // chunk, part, tsum_ref[...])
        de_buf[t] = jnp.dot(ut_ref[...], g_buf[...], preferred_element_type=jnp.float32)
        keep(t).start()

        @pl.when(t < tiles - held)
        def _():
            send_tile(t)

        return 0

    lax.fori_loop(0, tiles, step, 0)

    def to_core(q):
        rows = pl.ds(pl.multiple_of((2 * q + (1 - core)) * local, local), local)
        return pltpu.make_async_remote_copy(
            src_ref=du_ref.at[rows, :], dst_ref=core_buf.at[q], send_sem=red_send.at[q], recv_sem=red_recv.at[q],
            device_id=(tp, me ^ 1), device_id_type=MESH)

    for q in range(pairs):
        to_core(q).start()
    for q in range(pairs):
        to_core(q).wait()
    for q in range(pairs):
        core_buf[q] += du_ref[pl.ds(pl.multiple_of((2 * q + core) * local, local), local), :]

    def to_z(s):
        there = tp ^ s
        return pltpu.make_async_remote_copy(
            src_ref=core_buf.at[:, pl.ds(pl.multiple_of(there * part_rows, part_rows), part_rows), :], dst_ref=z_buf.at[s],
            send_sem=red_send.at[pairs + s], recv_sem=red_recv.at[pairs + s],
            device_id=(there, me), device_id_type=MESH)

    for s in range(1, groups):
        to_z(s).start()
    for s in range(1, groups):
        to_z(s).wait()
    mine = core_buf[:, pl.ds(pl.multiple_of(tp * part_rows, part_rows), part_rows), :]
    for s in range(1, groups):
        mine += z_buf[s]
    z_buf[0] = mine

    def to_chip(s):
        there = chip ^ s
        return pltpu.make_async_remote_copy(
            src_ref=z_buf.at[0, there], dst_ref=xy_buf.at[s],
            send_sem=red_send.at[pairs + groups + s], recv_sem=red_recv.at[pairs + groups + s],
            device_id=(tp, 2 * there + core), device_id_type=MESH)

    for s in range(1, pairs):
        to_chip(s).start()

    def late(t, _):
        send_tile(t)
        return 0

    lax.fori_loop(tiles - held, tiles, late, 0)
    for s in range(1, pairs):
        to_chip(s).wait()
    total = z_buf[0, chip]
    for s in range(1, pairs):
        total += xy_buf[s]
    tot_ref[...] = total
    here = pl.ds(pl.multiple_of(tp * part_rows, part_rows), part_rows)
    du_out[here, :] = total

    def share(s):
        return pltpu.make_async_remote_copy(
            src_ref=tot_ref, dst_ref=du_out.at[here, :],
            send_sem=red_send.at[2 * pairs + groups + s], recv_sem=red_recv.at[2 * pairs + groups + s],
            device_id=(tp ^ s, me), device_id_type=MESH)

    for s in range(1, groups):
        share(s).start()

    dw = jnp.sum(total * y_ref[here, :], axis=0, keepdims=True)
    rows = [dw[:, i * 128:(i + 1) * 128] for i in range(dim // 128)]
    rows.append(jnp.sum(tsum_ref[...], axis=0, keepdims=True))
    rows.append(jnp.zeros((16 - len(rows), 128), jnp.float32))
    sums = jnp.concatenate(rows, axis=0)
    mine_ref[...] = sums
    sums_ref[tp * peers + me] = sums
    start, wait = swap_all(mine_ref, sums_ref, all_send, all_recv, groups, peers)
    start()
    for s in range(1, groups):
        share(s).wait()
    du_full[...] = du_out[...]
    wait()
    sums_out[...] = jnp.sum(sums_ref[...], axis=0)

    def drain(t, _):
        keep(t).wait()
        for s in range(1, peers):
            send(t, s).wait()
        return 0

    lax.fori_loop(0, tiles, drain, 0)


def main_pass(emb, dense, u, ut, logz, w, y, groups, peers, tile=512, chunk=512, held=3):
    vocab, dim = emb.shape
    toks = u.shape[0]
    block = vocab // peers
    tiles = block // tile
    per = tile // LANES
    total = groups * peers
    local = toks // peers
    pairs = peers // 2
    f32 = jnp.float32
    vmem = pl.BlockSpec(memory_space=pltpu.VMEM)
    hbm = pl.BlockSpec(memory_space=pl.ANY)
    red = 2 * pairs + 2 * groups
    return pl.pallas_call(
        functools.partial(main_kernel, tile=tile, chunk=chunk, held=held, groups=groups, peers=peers),
        in_specs=[hbm, hbm, vmem, vmem, vmem, vmem, vmem],
        out_specs=[hbm, vmem, vmem],
        out_shape=[
            jax.ShapeDtypeStruct((dim // peers, vocab), f32),
            jax.ShapeDtypeStruct((local, dim), f32),
            jax.ShapeDtypeStruct((16, 128), f32),
        ],
        scratch_shapes=[
            pltpu.VMEM((2, tile, dim), jnp.bfloat16),
            pltpu.VMEM((2, per, toks, LANES), f32),
            pltpu.VMEM((toks, tile), jnp.bfloat16),
            pltpu.VMEM((tiles, dim, tile), f32),
            pltpu.VMEM((toks, dim), f32),
            pltpu.VMEM((8, LANES), f32),
            pltpu.VMEM((pairs, local, dim), f32),
            pltpu.VMEM((groups, pairs, local // groups, dim), f32),
            pltpu.VMEM((pairs, local // groups, dim), f32),
            pltpu.VMEM((local // groups, dim), f32),
            pltpu.VMEM((16, 128), f32),
            pltpu.VMEM((local, dim), f32),
            pltpu.VMEM((total, 16, 128), f32),
            pltpu.SemaphoreType.DMA((2, 2)),
            pltpu.SemaphoreType.DMA((tiles, peers)),
            pltpu.SemaphoreType.DMA((tiles, peers)),
            pltpu.SemaphoreType.DMA((tiles,)),
            pltpu.SemaphoreType.DMA((red,)),
            pltpu.SemaphoreType.DMA((red,)),
            pltpu.SemaphoreType.DMA((total,)),
            pltpu.SemaphoreType.DMA((total,)),
        ],
        compiler_params=pltpu.CompilerParams(vmem_limit_bytes=63 * MIB, collective_id=0, has_side_effects=True),
        cost_estimate=pl.CostEstimate(flops=6 * block * dim * toks, bytes_accessed=4 * block * toks, transcendentals=block * toks),
    )(emb, dense, u, ut, logz, w, y)


def solution(mesh):
    peers = mesh.shape['dp']
    groups = mesh.shape['tp']

    def local_head(hidden, embedding, norm_weight, teach_ids, teach_prob, tok_mask):
        vocab_local = embedding.shape[0]
        toks = hidden.shape[0]
        block = vocab_local // peers
        high = block // LANES
        dim = hidden.shape[1]
        tp = lax.axis_index('tp')
        dp = lax.axis_index('dp')
        scale_w = 1.0 + norm_weight
        h_f32 = hidden.astype(jnp.float32)
        inv_rms = lax.rsqrt(jnp.mean(h_f32 * h_f32, axis=1, keepdims=True) + EPS_NORM)
        normed = h_f32 * inv_rms

        ids_all = lax.all_gather(teach_ids, 'dp', axis=0, tiled=True)
        prob_all = lax.all_gather(teach_prob, 'dp', axis=0, tiled=True)
        normed_all = lax.all_gather(normed, 'dp', axis=0, tiled=True)

        u_loc = (normed * scale_w).astype(jnp.bfloat16)
        stats = local_stats(embedding, u_loc.T, tok_mask.reshape(1, -1), groups, peers)
        stats = stats.reshape(groups, peers, 8, toks)
        row_max = jnp.max(stats[:, :, 0], axis=0)
        sum_exp = jnp.sum(stats[:, :, 1] * jnp.exp(stats[:, :, 0] - row_max), axis=0)
        log_norm = (row_max + jnp.log(sum_exp)).reshape(-1, 1)
        mask = stats[0, :, 2].reshape(-1, 1)
        weight = mask / jnp.sum(mask)

        base = (tp * vocab_local + dp * block).astype(jnp.int32).reshape(1)
        dense = teacher_dense(base, ids_all, prob_all, high)
        u_all = (normed_all * scale_w).astype(jnp.bfloat16)
        de_t, grad_u, sums = main_pass(embedding, dense, u_all, u_all.T, log_norm, weight, normed, groups, peers)
        used = dim // 128
        grad_norm = sums[:used].reshape(dim)
        loss_mean = jnp.sum(weight * log_norm) - jnp.sum(sums[used])
        d_normed = grad_u * scale_w
        grad_hidden = (inv_rms * (d_normed - normed * jnp.mean(d_normed * normed, axis=1, keepdims=True))).astype(jnp.bfloat16)
        return loss_mean, grad_hidden, de_t.T, grad_norm

    return jax.shard_map(local_head, mesh=mesh, in_specs=(P('dp', None), P('tp', None), P(None), P('dp', None), P('dp', None), P('dp')), out_specs=(P(), P('dp', None), P('tp', 'dp'), P(None)), check_vma=False)
```

```python
import functools

import jax
import jax.numpy as jnp
from jax import lax
from jax.experimental import pallas as pl
from jax.experimental.pallas import tpu as pltpu
from jax.sharding import PartitionSpec as P

EPS_NORM = 1e-6
LANES = 128
TILE = 512
OWN = 8
MIB = 1024 * 1024
NT = (((1,), (1,)), ((), ()))
MESH = pl.DeviceIdType.MESH


def swap_all(src, dst, send_sem, recv_sem, groups, peers):
    total = groups * peers
    me = lax.axis_index('tp') * peers + lax.axis_index('dp')

    def copy(s):
        to = lax.rem(me + s, total)
        return pltpu.make_async_remote_copy(
            src_ref=src, dst_ref=dst.at[me], send_sem=send_sem.at[s], recv_sem=recv_sem.at[s],
            device_id=(to // peers, lax.rem(to, peers)), device_id_type=MESH)

    def start(s, _):
        copy(s).start()
        return 0

    def wait(s, _):
        copy(s).wait()
        return 0

    return (lambda: lax.fori_loop(1, total, start, 0)), (lambda: lax.fori_loop(1, total, wait, 0))


def enter_all(groups, peers):
    total = groups * peers
    me = lax.axis_index('tp') * peers + lax.axis_index('dp')
    barrier = pltpu.get_barrier_semaphore()

    def greet(s, _):
        to = lax.rem(me + s, total)
        pl.semaphore_signal(barrier, inc=1, device_id=(to // peers, lax.rem(to, peers)), device_id_type=MESH)
        return 0

    lax.fori_loop(1, total, greet, 0)
    pl.semaphore_wait(barrier, total - 1)


def stats_kernel(emb_ref, ut_ref, mask_ref, out_ref, max_ref, sum_ref, mine_ref, all_ref, send_sem, recv_sem, *, sub, groups, peers):
    @pl.when(pl.program_id(0) == 0)
    def _():
        max_ref[...] = jnp.full(max_ref.shape, -jnp.inf, jnp.float32)
        sum_ref[...] = jnp.zeros(sum_ref.shape, jnp.float32)

    rows = emb_ref.shape[0]
    toks = ut_ref.shape[1]
    for c in range(rows // sub):
        z = jnp.dot(emb_ref[c * sub:(c + 1) * sub, :], ut_ref[...], preferred_element_type=jnp.float32)
        z = z.reshape(sub // 8, 8, toks)
        old = max_ref[...]
        new = jnp.maximum(old, jnp.max(z, axis=0))
        sum_ref[...] = sum_ref[...] * jnp.exp(old - new) + jnp.sum(jnp.exp(z - new[None]), axis=0)
        max_ref[...] = new

    @pl.when(pl.program_id(0) == pl.num_programs(0) - 1)
    def _():
        top = jnp.max(max_ref[...], axis=0, keepdims=True)
        tot = jnp.sum(sum_ref[...] * jnp.exp(max_ref[...] - top), axis=0, keepdims=True)
        row = lax.broadcasted_iota(jnp.int32, (8, toks), 0)
        mine = jnp.where(row == 0, top, jnp.where(row == 1, tot, mask_ref[...]))
        mine_ref[...] = mine
        me = lax.axis_index('tp') * peers + lax.axis_index('dp')
        all_ref[me] = mine
        enter_all(groups, peers)
        start, wait = swap_all(mine_ref, all_ref, send_sem, recv_sem, groups, peers)
        start()
        wait()
        out_ref[...] = all_ref[...]


def local_stats(emb, ut, mask, groups, peers, rows=8192, sub=1024):
    vocab, dim = emb.shape
    toks = ut.shape[1]
    total = groups * peers
    return pl.pallas_call(
        functools.partial(stats_kernel, sub=sub, groups=groups, peers=peers),
        grid=(vocab // rows,),
        in_specs=[pl.BlockSpec((rows, dim), lambda i: (i, 0)), pl.BlockSpec((dim, toks), lambda i: (0, 0)), pl.BlockSpec((1, toks), lambda i: (0, 0))],
        out_specs=pl.BlockSpec((total, 8, toks), lambda i: (0, 0, 0)),
        out_shape=jax.ShapeDtypeStruct((total, 8, toks), jnp.float32),
        scratch_shapes=[pltpu.VMEM((8, toks), jnp.float32)] * 3 + [pltpu.VMEM((total, 8, toks), jnp.float32)] + [pltpu.SemaphoreType.DMA((total,))] * 2,
        compiler_params=pltpu.CompilerParams(vmem_limit_bytes=40 * MIB, collective_id=1, has_side_effects=True),
        cost_estimate=pl.CostEstimate(flops=2 * vocab * dim * toks, bytes_accessed=2 * vocab * dim, transcendentals=vocab * toks),
    )(emb, ut, mask)


def teacher_kernel(base_ref, ids_ref, prob_ref, out_ref, *, regions, group):
    top = ids_ref.shape[1]
    high = sum(regions)
    bf16 = jnp.bfloat16
    high_iota = lax.broadcasted_iota(jnp.int32, (high, top), 0).astype(jnp.float32).astype(bf16)
    low_iota = lax.broadcasted_iota(jnp.int32, (LANES, top), 0).astype(jnp.float32).astype(bf16)

    def spread(row, n):
        row = jnp.broadcast_to(row, (16, top)).astype(bf16)
        return jnp.broadcast_to(row[None], (n // 16, 16, top)).reshape(n, top)

    def step(i, _):
        rows = pl.ds(pl.multiple_of(i * group, group), group)
        ids = ids_ref[rows, :]
        lo = (ids & (LANES - 1)).astype(jnp.float32)
        hi = jnp.full(ids.shape, -1, jnp.int32)
        first = 0
        for r, size in enumerate(regions):
            local = (ids >> (LANES.bit_length() - 1)) - base_ref[r]
            hi = jnp.where((local >= 0) & (local < size), local + first, hi)
            first += size
        hi = hi.astype(jnp.float32)
        prob = prob_ref[rows, :]
        p1 = prob.astype(bf16).astype(jnp.float32)
        r1 = prob - p1
        p2 = r1.astype(bf16).astype(jnp.float32)
        p3 = r1 - p2
        parts = []
        for j in range(group):
            hit = high_iota == spread(hi[j:j + 1, :], high)
            left = [jnp.where(hit, spread(p[j:j + 1, :], high), jnp.zeros((), bf16)) for p in (p1, p2, p3)]
            right = jnp.where(low_iota == spread(lo[j:j + 1, :], LANES), jnp.ones((), bf16), jnp.zeros((), bf16))
            dense = lax.dot_general(jnp.concatenate(left, axis=0), right, NT, preferred_element_type=jnp.float32)
            parts.append(dense[:high] + (dense[high:2 * high] + dense[2 * high:]))
        out_ref[:, rows, :] = jnp.swapaxes(jnp.stack(parts, axis=0), 0, 1)
        return 0

    lax.fori_loop(0, ids_ref.shape[0] // group, step, 0)


def teacher_dense(base, ids, prob, regions, block=128):
    high = sum(regions)
    toks, top = ids.shape
    return pl.pallas_call(
        functools.partial(teacher_kernel, regions=regions, group=64),
        grid=(toks // block,),
        in_specs=[pl.BlockSpec(memory_space=pltpu.SMEM), pl.BlockSpec((block, top), lambda i: (i, 0)), pl.BlockSpec((block, top), lambda i: (i, 0))],
        out_specs=pl.BlockSpec((high, block, LANES), lambda i: (0, i, 0)),
        out_shape=jax.ShapeDtypeStruct((high, toks, LANES), jnp.float32),
        compiler_params=pltpu.CompilerParams(vmem_limit_bytes=40 * MIB),
        cost_estimate=pl.CostEstimate(flops=6 * high * LANES * toks * top, bytes_accessed=4 * high * LANES * toks, transcendentals=0),
    )(base, ids, prob)


def main_kernel(emb, dense, u_ref, ut_ref, logz_ref, w_ref, y_ref, out, du_full, sums_out,
                emb_buf, dense_buf, g_buf, ut_half, de_buf, de_half, du_ref, tsum_ref, core_buf, z_buf, xy_buf, tot_ref, mine_ref, du_out, sums_ref,
                in_sem, send_sem, recv_sem, own_sem, half_send, half_recv, half_own, red_send, red_recv, all_send, all_recv,
                *, tile, own, shared, held, groups, peers):
    toks, dim = u_ref.shape
    cols = dim // peers
    local = toks // peers
    part_rows = local // groups
    tp = lax.axis_index('tp')
    me = lax.axis_index('dp')
    per = tile // LANES
    pairs = peers // 2
    core = lax.rem(me, 2)
    chip = me // 2
    x_pos = lax.rem(chip, 2)
    y_pos = chip // 2
    chunk = toks // 2
    wide = dim // 2

    enter_all(groups, peers)

    def first_row(k, i):
        index = (me * own, peers * own + (2 * y_pos + core) * shared, peers * own + pairs * shared + (2 * x_pos + core) * shared)[k]
        return pl.multiple_of((index + i) * tile, tile)

    def fetch(k, i, slot):
        plane = ((0, own, own + shared)[k] + i) * per
        return (
            pltpu.make_async_copy(emb.at[pl.ds(first_row(k, i), tile), :], emb_buf.at[slot], in_sem.at[slot, 0]),
            pltpu.make_async_copy(dense.at[pl.ds(plane, per)], dense_buf.at[slot], in_sem.at[slot, 1]),
        )

    def begin(k, i, slot):
        for c in fetch(k, i, slot):
            c.start()

    def arrive(k, i, slot):
        for c in fetch(k, i, slot):
            c.wait()

    def send(i, s):
        to = me ^ s
        return pltpu.make_async_remote_copy(
            src_ref=de_buf.at[i, pl.ds(pl.multiple_of(to * cols, 8), cols), :],
            dst_ref=out.at[:, pl.ds(first_row(0, i), tile)],
            send_sem=send_sem.at[i, s], recv_sem=recv_sem.at[i, s],
            device_id=(tp, to), device_id_type=MESH)

    def keep(i):
        return pltpu.make_async_copy(
            de_buf.at[i, pl.ds(pl.multiple_of(me * cols, 8), cols), :],
            out.at[:, pl.ds(first_row(0, i), tile)], own_sem.at[i])

    def place(k, dev):
        far = dev // pairs if k == 1 else lax.rem(dev // 2, 2)
        return pl.multiple_of((2 * far + lax.rem(dev, 2)) * cols, 8)

    def send_half(k, i, s):
        to = me ^ ((s & 1) + (s >> 1) * (pairs if k == 1 else 2))
        return pltpu.make_async_remote_copy(
            src_ref=de_half.at[k - 1, i, pl.ds(place(k, to), cols), :],
            dst_ref=out.at[:, pl.ds(first_row(k, i), tile)],
            send_sem=half_send.at[k - 1, i, s], recv_sem=half_recv.at[k - 1, i, s],
            device_id=(tp, to), device_id_type=MESH)

    def keep_half(k, i):
        return pltpu.make_async_copy(
            de_half.at[k - 1, i, pl.ds(place(k, me), cols), :],
            out.at[:, pl.ds(first_row(k, i), tile)], half_own.at[k - 1, i])

    begin(0, 0, 0)
    du_ref[...] = jnp.zeros(du_ref.shape, jnp.float32)
    tsum_ref[...] = jnp.zeros(tsum_ref.shape, jnp.float32)
    quarter = dim // 4
    for j in range(2):
        lines = pl.ds(pl.multiple_of(j * wide + x_pos * quarter, 16), quarter)
        ut_half[0, j * quarter:(j + 1) * quarter, :] = ut_ref[lines, :]
    ut_half[1] = ut_ref[pl.ds(pl.multiple_of(y_pos * wide, 16), wide), :]

    def gradient(rows, slot, counted):
        e = emb_buf[slot]
        z = lax.dot_general(u_ref[rows, :], e, NT, preferred_element_type=jnp.float32)
        w = w_ref[rows, :]
        logz = logz_ref[rows, :]
        acc = jnp.zeros((8, LANES), jnp.float32)
        for h in range(per):
            zh = z[:, h * LANES:(h + 1) * LANES]
            q = dense_buf[slot, h, rows, :] * w
            g_buf[rows, h * LANES:(h + 1) * LANES] = (jnp.exp(zh - logz) * w - q).astype(jnp.bfloat16)
            if counted:
                acc = acc + jnp.sum((q * zh).reshape(chunk // 8, 8, LANES), axis=0)
        if counted:
            tsum_ref[...] += acc
            du_ref[rows, :] += jnp.dot(g_buf[rows, :], e, preferred_element_type=jnp.float32)

    def own_step(i, _):
        slot = lax.rem(i, 2)
        arrive(0, i, slot)

        @pl.when(i + 1 < own)
        def _():
            begin(0, i + 1, 1 - slot)

        @pl.when(i + 1 == own)
        def _():
            begin(1, 0, 0)

        def part(c, _):
            gradient(pl.ds(pl.multiple_of(c * chunk, chunk), chunk), slot, True)
            return 0

        lax.fori_loop(0, 2, part, 0)
        de_buf[i] = jnp.dot(ut_ref[...], g_buf[...], preferred_element_type=jnp.float32)
        keep(i).start()
        for s in range(peers - 1, 0, -1):
            send(i, s).start()
        return 0

    lax.fori_loop(0, own, own_step, 0)

    def send_shared(i):
        for k in (1, 2):
            for s in (3, 2, 1):
                send_half(k, i, s).start()

    def shared_step(i, _):
        for k, half in ((1, x_pos), (2, y_pos)):
            slot = k - 1
            arrive(k, i, slot)
            if k == 1:
                begin(2, i, 1)
            else:
                @pl.when(i + 1 < shared)
                def _():
                    begin(1, i + 1, 0)
            gradient(pl.ds(pl.multiple_of((1 - half) * chunk, chunk), chunk), slot, False)
            gradient(pl.ds(pl.multiple_of(half * chunk, chunk), chunk), slot, True)
            de_half[k - 1, i] = jnp.dot(ut_half[k - 1], g_buf[...], preferred_element_type=jnp.float32)
            keep_half(k, i).start()

        @pl.when(i < shared - held)
        def _():
            send_shared(i)

        return 0

    lax.fori_loop(0, shared, shared_step, 0)

    def to_core(q):
        rows = pl.ds(pl.multiple_of((2 * q + (1 - core)) * local, local), local)
        return pltpu.make_async_remote_copy(
            src_ref=du_ref.at[rows, :], dst_ref=core_buf.at[q], send_sem=red_send.at[q], recv_sem=red_recv.at[q],
            device_id=(tp, me ^ 1), device_id_type=MESH)

    for q in range(pairs):
        to_core(q).start()
    for q in range(pairs):
        to_core(q).wait()
    for q in range(pairs):
        core_buf[q] += du_ref[pl.ds(pl.multiple_of((2 * q + core) * local, local), local), :]

    def to_z(s):
        there = tp ^ s
        return pltpu.make_async_remote_copy(
            src_ref=core_buf.at[:, pl.ds(pl.multiple_of(there * part_rows, part_rows), part_rows), :], dst_ref=z_buf.at[s],
            send_sem=red_send.at[pairs + s], recv_sem=red_recv.at[pairs + s],
            device_id=(there, me), device_id_type=MESH)

    for s in range(1, groups):
        to_z(s).start()
    for s in range(1, groups):
        to_z(s).wait()
    mine = core_buf[:, pl.ds(pl.multiple_of(tp * part_rows, part_rows), part_rows), :]
    for s in range(1, groups):
        mine += z_buf[s]
    z_buf[0] = mine

    def to_chip(s):
        there = chip ^ s
        return pltpu.make_async_remote_copy(
            src_ref=z_buf.at[0, there], dst_ref=xy_buf.at[s],
            send_sem=red_send.at[pairs + groups + s], recv_sem=red_recv.at[pairs + groups + s],
            device_id=(tp, 2 * there + core), device_id_type=MESH)

    for s in range(1, pairs):
        to_chip(s).start()

    def late(i, _):
        send_shared(i)
        return 0

    lax.fori_loop(shared - held, shared, late, 0)
    for s in range(1, pairs):
        to_chip(s).wait()
    total = z_buf[0, chip]
    for s in range(1, pairs):
        total += xy_buf[s]
    tot_ref[...] = total
    here = pl.ds(pl.multiple_of(tp * part_rows, part_rows), part_rows)
    du_out[here, :] = total

    def share(s):
        return pltpu.make_async_remote_copy(
            src_ref=tot_ref, dst_ref=du_out.at[here, :],
            send_sem=red_send.at[2 * pairs + groups + s], recv_sem=red_recv.at[2 * pairs + groups + s],
            device_id=(tp ^ s, me), device_id_type=MESH)

    for s in range(1, groups):
        share(s).start()

    dw = jnp.sum(total * y_ref[here, :], axis=0, keepdims=True)
    rows = [dw[:, i * 128:(i + 1) * 128] for i in range(dim // 128)]
    rows.append(jnp.sum(tsum_ref[...], axis=0, keepdims=True))
    rows.append(jnp.zeros((16 - len(rows), 128), jnp.float32))
    sums = jnp.concatenate(rows, axis=0)
    mine_ref[...] = sums
    sums_ref[tp * peers + me] = sums
    start, wait = swap_all(mine_ref, sums_ref, all_send, all_recv, groups, peers)
    start()
    for s in range(1, groups):
        share(s).wait()
    du_full[...] = du_out[...]
    wait()
    sums_out[...] = jnp.sum(sums_ref[...], axis=0)

    def drain(i, _):
        keep(i).wait()
        for s in range(1, peers):
            send(i, s).wait()
        return 0

    lax.fori_loop(0, own, drain, 0)

    def drain_half(i, _):
        for k in (1, 2):
            keep_half(k, i).wait()
            for s in (1, 2, 3):
                send_half(k, i, s).wait()
        return 0

    lax.fori_loop(0, shared, drain_half, 0)


def main_pass(emb, dense, u, ut, logz, w, y, own, shared, groups, peers, tile=TILE, held=2):
    vocab, dim = emb.shape
    toks = u.shape[0]
    per = tile // LANES
    total = groups * peers
    local = toks // peers
    pairs = peers // 2
    f32 = jnp.float32
    vmem = pl.BlockSpec(memory_space=pltpu.VMEM)
    hbm = pl.BlockSpec(memory_space=pl.ANY)
    red = 2 * pairs + 2 * groups
    return pl.pallas_call(
        functools.partial(main_kernel, tile=tile, own=own, shared=shared, held=held, groups=groups, peers=peers),
        in_specs=[hbm, hbm, vmem, vmem, vmem, vmem, vmem],
        out_specs=[hbm, vmem, vmem],
        out_shape=[
            jax.ShapeDtypeStruct((dim // peers, vocab), f32),
            jax.ShapeDtypeStruct((local, dim), f32),
            jax.ShapeDtypeStruct((16, 128), f32),
        ],
        scratch_shapes=[
            pltpu.VMEM((2, tile, dim), jnp.bfloat16),
            pltpu.VMEM((2, per, toks, LANES), f32),
            pltpu.VMEM((toks, tile), jnp.bfloat16),
            pltpu.VMEM((2, dim // 2, toks), jnp.bfloat16),
            pltpu.VMEM((own, dim, tile), f32),
            pltpu.VMEM((2, shared, dim // 2, tile), f32),
            pltpu.VMEM((toks, dim), f32),
            pltpu.VMEM((8, LANES), f32),
            pltpu.VMEM((pairs, local, dim), f32),
            pltpu.VMEM((groups, pairs, local // groups, dim), f32),
            pltpu.VMEM((pairs, local // groups, dim), f32),
            pltpu.VMEM((local // groups, dim), f32),
            pltpu.VMEM((16, 128), f32),
            pltpu.VMEM((local, dim), f32),
            pltpu.VMEM((total, 16, 128), f32),
            pltpu.SemaphoreType.DMA((2, 2)),
            pltpu.SemaphoreType.DMA((own, peers)),
            pltpu.SemaphoreType.DMA((own, peers)),
            pltpu.SemaphoreType.DMA((own,)),
            pltpu.SemaphoreType.DMA((2, shared, 4)),
            pltpu.SemaphoreType.DMA((2, shared, 4)),
            pltpu.SemaphoreType.DMA((2, shared)),
            pltpu.SemaphoreType.DMA((red,)),
            pltpu.SemaphoreType.DMA((red,)),
            pltpu.SemaphoreType.DMA((total,)),
            pltpu.SemaphoreType.DMA((total,)),
        ],
        compiler_params=pltpu.CompilerParams(vmem_limit_bytes=63 * MIB, collective_id=0, has_side_effects=True),
        cost_estimate=pl.CostEstimate(flops=6 * vocab // peers * dim * toks, bytes_accessed=4 * vocab // peers * toks, transcendentals=vocab // peers * toks),
    )(emb, dense, u, ut, logz, w, y)


def solution(mesh):
    peers = mesh.shape['dp']
    groups = mesh.shape['tp']

    def local_head(hidden, embedding, norm_weight, teach_ids, teach_prob, tok_mask):
        vocab_local = embedding.shape[0]
        toks = hidden.shape[0]
        dim = hidden.shape[1]
        tp = lax.axis_index('tp')
        dp = lax.axis_index('dp')
        scale_w = 1.0 + norm_weight
        h_f32 = hidden.astype(jnp.float32)
        inv_rms = lax.rsqrt(jnp.mean(h_f32 * h_f32, axis=1, keepdims=True) + EPS_NORM)
        normed = h_f32 * inv_rms

        ids_all = lax.all_gather(teach_ids, 'dp', axis=0, tiled=True)
        prob_all = lax.all_gather(teach_prob, 'dp', axis=0, tiled=True)
        normed_all = lax.all_gather(normed, 'dp', axis=0, tiled=True)

        u_loc = (normed * scale_w).astype(jnp.bfloat16)
        stats = local_stats(embedding, u_loc.T, tok_mask.reshape(1, -1), groups, peers)
        stats = stats.reshape(groups, peers, 8, toks)
        row_max = jnp.max(stats[:, :, 0], axis=0)
        sum_exp = jnp.sum(stats[:, :, 1] * jnp.exp(stats[:, :, 0] - row_max), axis=0)
        log_norm = (row_max + jnp.log(sum_exp)).reshape(-1, 1)
        mask = stats[0, :, 2].reshape(-1, 1)
        weight = mask / jnp.sum(mask)

        tiles = vocab_local // TILE
        own = OWN
        shared = tiles // peers - own
        core, chip = dp % 2, dp // 2
        starts = [dp * own, peers * own + (2 * (chip // 2) + core) * shared, peers * own + (peers // 2) * shared + (2 * (chip % 2) + core) * shared]
        base = (jnp.stack(starts) * (TILE // LANES) + tp * (vocab_local // LANES)).astype(jnp.int32)
        regions = tuple(n * (TILE // LANES) for n in (own, shared, shared))
        dense = teacher_dense(base, ids_all, prob_all, regions)
        u_all = (normed_all * scale_w).astype(jnp.bfloat16)
        de_t, grad_u, sums = main_pass(embedding, dense, u_all, u_all.T, log_norm, weight, normed, own, shared, groups, peers)
        used = dim // 128
        grad_norm = sums[:used].reshape(dim)
        loss_mean = jnp.sum(weight * log_norm) - jnp.sum(sums[used])
        d_normed = grad_u * scale_w
        grad_hidden = (inv_rms * (d_normed - normed * jnp.mean(d_normed * normed, axis=1, keepdims=True))).astype(jnp.bfloat16)
        return loss_mean, grad_hidden, de_t.T, grad_norm

    return jax.shard_map(local_head, mesh=mesh, in_specs=(P('dp', None), P('tp', None), P(None), P('dp', None), P('dp', None), P('dp')), out_specs=(P(), P('dp', None), P('tp', 'dp'), P(None)), check_vma=False)
```

```python
import functools

import jax
import jax.numpy as jnp
from jax import lax
from jax.experimental import pallas as pl
from jax.experimental.pallas import tpu as pltpu
from jax.sharding import PartitionSpec as P

EPS_NORM = 1e-6
LANES = 128
TILE = 512
OWN = 8
HELD = 3
MIB = 1024 * 1024
NT = (((1,), (1,)), ((), ()))
MESH = pl.DeviceIdType.MESH


def swap_all(src, dst, send_sem, recv_sem, groups, peers):
    total = groups * peers
    me = lax.axis_index('tp') * peers + lax.axis_index('dp')

    def copy(s):
        to = lax.rem(me + s, total)
        return pltpu.make_async_remote_copy(
            src_ref=src, dst_ref=dst.at[me], send_sem=send_sem.at[s], recv_sem=recv_sem.at[s],
            device_id=(to // peers, lax.rem(to, peers)), device_id_type=MESH)

    def start(s, _):
        copy(s).start()
        return 0

    def wait(s, _):
        copy(s).wait()
        return 0

    return (lambda: lax.fori_loop(1, total, start, 0)), (lambda: lax.fori_loop(1, total, wait, 0))


def enter_all(groups, peers):
    total = groups * peers
    me = lax.axis_index('tp') * peers + lax.axis_index('dp')
    barrier = pltpu.get_barrier_semaphore()

    def greet(s, _):
        to = lax.rem(me + s, total)
        pl.semaphore_signal(barrier, inc=1, device_id=(to // peers, lax.rem(to, peers)), device_id_type=MESH)
        return 0

    lax.fori_loop(1, total, greet, 0)
    pl.semaphore_wait(barrier, total - 1)


def stats_kernel(emb_ref, ut_ref, mask_ref, out_ref, max_ref, sum_ref, mine_ref, all_ref, send_sem, recv_sem, *, sub, groups, peers):
    @pl.when(pl.program_id(0) == 0)
    def _():
        max_ref[...] = jnp.full(max_ref.shape, -jnp.inf, jnp.float32)
        sum_ref[...] = jnp.zeros(sum_ref.shape, jnp.float32)

    rows = emb_ref.shape[0]
    toks = ut_ref.shape[1]
    for c in range(rows // sub):
        z = jnp.dot(emb_ref[c * sub:(c + 1) * sub, :], ut_ref[...], preferred_element_type=jnp.float32)
        z = z.reshape(sub // 8, 8, toks)
        old = max_ref[...]
        new = jnp.maximum(old, jnp.max(z, axis=0))
        sum_ref[...] = sum_ref[...] * jnp.exp(old - new) + jnp.sum(jnp.exp(z - new[None]), axis=0)
        max_ref[...] = new

    @pl.when(pl.program_id(0) == pl.num_programs(0) - 1)
    def _():
        top = jnp.max(max_ref[...], axis=0, keepdims=True)
        tot = jnp.sum(sum_ref[...] * jnp.exp(max_ref[...] - top), axis=0, keepdims=True)
        row = lax.broadcasted_iota(jnp.int32, (8, toks), 0)
        mine = jnp.where(row == 0, top, jnp.where(row == 1, tot, mask_ref[...]))
        mine_ref[...] = mine
        me = lax.axis_index('tp') * peers + lax.axis_index('dp')
        all_ref[me] = mine
        enter_all(groups, peers)
        start, wait = swap_all(mine_ref, all_ref, send_sem, recv_sem, groups, peers)
        start()
        wait()
        out_ref[...] = all_ref[...]


def local_stats(emb, ut, mask, groups, peers, rows=8192, sub=1024):
    vocab, dim = emb.shape
    toks = ut.shape[1]
    total = groups * peers
    return pl.pallas_call(
        functools.partial(stats_kernel, sub=sub, groups=groups, peers=peers),
        grid=(vocab // rows,),
        in_specs=[pl.BlockSpec((rows, dim), lambda i: (i, 0)), pl.BlockSpec((dim, toks), lambda i: (0, 0)), pl.BlockSpec((1, toks), lambda i: (0, 0))],
        out_specs=pl.BlockSpec((total, 8, toks), lambda i: (0, 0, 0)),
        out_shape=jax.ShapeDtypeStruct((total, 8, toks), jnp.float32),
        scratch_shapes=[pltpu.VMEM((8, toks), jnp.float32)] * 3 + [pltpu.VMEM((total, 8, toks), jnp.float32)] + [pltpu.SemaphoreType.DMA((total,))] * 2,
        compiler_params=pltpu.CompilerParams(vmem_limit_bytes=40 * MIB, collective_id=1, has_side_effects=True),
        cost_estimate=pl.CostEstimate(flops=2 * vocab * dim * toks, bytes_accessed=2 * vocab * dim, transcendentals=vocab * toks),
    )(emb, ut, mask)


def teacher_kernel(base_ref, ids_ref, prob_ref, out_ref, *, regions, group):
    top = ids_ref.shape[1]
    high = sum(regions)
    bf16 = jnp.bfloat16
    high_iota = lax.broadcasted_iota(jnp.int32, (high, top), 0).astype(jnp.float32).astype(bf16)
    low_iota = lax.broadcasted_iota(jnp.int32, (LANES, top), 0).astype(jnp.float32).astype(bf16)

    def spread(row, n):
        row = jnp.broadcast_to(row, (16, top)).astype(bf16)
        return jnp.broadcast_to(row[None], (n // 16, 16, top)).reshape(n, top)

    def step(i, _):
        rows = pl.ds(pl.multiple_of(i * group, group), group)
        ids = ids_ref[rows, :]
        lo = (ids & (LANES - 1)).astype(jnp.float32)
        hi = jnp.full(ids.shape, -1, jnp.int32)
        first = 0
        for r, size in enumerate(regions):
            local = (ids >> (LANES.bit_length() - 1)) - base_ref[r]
            hi = jnp.where((local >= 0) & (local < size), local + first, hi)
            first += size
        hi = hi.astype(jnp.float32)
        prob = prob_ref[rows, :]
        p1 = prob.astype(bf16).astype(jnp.float32)
        r1 = prob - p1
        p2 = r1.astype(bf16).astype(jnp.float32)
        p3 = r1 - p2
        parts = []
        for j in range(group):
            hit = high_iota == spread(hi[j:j + 1, :], high)
            left = [jnp.where(hit, spread(p[j:j + 1, :], high), jnp.zeros((), bf16)) for p in (p1, p2, p3)]
            right = jnp.where(low_iota == spread(lo[j:j + 1, :], LANES), jnp.ones((), bf16), jnp.zeros((), bf16))
            dense = lax.dot_general(jnp.concatenate(left, axis=0), right, NT, preferred_element_type=jnp.float32)
            parts.append(dense[:high] + (dense[high:2 * high] + dense[2 * high:]))
        out_ref[:, rows, :] = jnp.swapaxes(jnp.stack(parts, axis=0), 0, 1)
        return 0

    lax.fori_loop(0, ids_ref.shape[0] // group, step, 0)


def teacher_dense(base, ids, prob, regions, block=128):
    high = sum(regions)
    toks, top = ids.shape
    return pl.pallas_call(
        functools.partial(teacher_kernel, regions=regions, group=64),
        grid=(toks // block,),
        in_specs=[pl.BlockSpec(memory_space=pltpu.SMEM), pl.BlockSpec((block, top), lambda i: (i, 0)), pl.BlockSpec((block, top), lambda i: (i, 0))],
        out_specs=pl.BlockSpec((high, block, LANES), lambda i: (0, i, 0)),
        out_shape=jax.ShapeDtypeStruct((high, toks, LANES), jnp.float32),
        compiler_params=pltpu.CompilerParams(vmem_limit_bytes=40 * MIB),
        cost_estimate=pl.CostEstimate(flops=6 * high * LANES * toks * top, bytes_accessed=4 * high * LANES * toks, transcendentals=0),
    )(base, ids, prob)


def main_kernel(emb, dense, u_ref, ut_ref, logz_ref, w_ref, y_ref, out, g_keep, du_full, sums_out,
                emb_buf, dense_buf, g_buf, ut_half, de_buf, de_half, du_ref, tsum_ref, core_buf, z_buf, xy_buf, tot_ref, mine_ref, du_out, sums_ref,
                in_sem, g_put, g_get, send_sem, recv_sem, own_sem, half_send, half_recv, half_own, red_send, red_recv, all_send, all_recv,
                *, tile, own, shared, held, groups, peers):
    toks, dim = u_ref.shape
    cols = dim // peers
    local = toks // peers
    part_rows = local // groups
    tp = lax.axis_index('tp')
    me = lax.axis_index('dp')
    per = tile // LANES
    pairs = peers // 2
    core = lax.rem(me, 2)
    chip = me // 2
    x_pos = lax.rem(chip, 2)
    y_pos = chip // 2
    chunk = toks // 2
    wide = dim // 2

    enter_all(groups, peers)

    def first_row(k, i):
        index = (me * own, peers * own + (2 * y_pos + core) * shared, peers * own + pairs * shared + (2 * x_pos + core) * shared)[k]
        return pl.multiple_of((index + i) * tile, tile)

    def fetch(k, i, slot):
        plane = ((0, own, own + shared)[k] + i) * per
        return (
            pltpu.make_async_copy(emb.at[pl.ds(first_row(k, i), tile), :], emb_buf.at[slot], in_sem.at[slot, 0]),
            pltpu.make_async_copy(dense.at[pl.ds(plane, per)], dense_buf.at[slot], in_sem.at[slot, 1]),
        )

    def begin(k, i, slot):
        for c in fetch(k, i, slot):
            c.start()

    def arrive(k, i, slot):
        for c in fetch(k, i, slot):
            c.wait()

    def send(i, s):
        to = me ^ s
        return pltpu.make_async_remote_copy(
            src_ref=de_buf.at[i, pl.ds(pl.multiple_of(to * cols, 8), cols), :],
            dst_ref=out.at[:, pl.ds(first_row(0, i), tile)],
            send_sem=send_sem.at[i, s], recv_sem=recv_sem.at[i, s],
            device_id=(tp, to), device_id_type=MESH)

    def keep(i):
        return pltpu.make_async_copy(
            de_buf.at[i, pl.ds(pl.multiple_of(me * cols, 8), cols), :],
            out.at[:, pl.ds(first_row(0, i), tile)], own_sem.at[i])

    def place(k, dev):
        far = dev // pairs if k == 1 else lax.rem(dev // 2, 2)
        return pl.multiple_of((2 * far + lax.rem(dev, 2)) * cols, 8)

    def send_half(k, i, s):
        to = me ^ ((s & 1) + (s >> 1) * (pairs if k == 1 else 2))
        return pltpu.make_async_remote_copy(
            src_ref=de_half.at[k - 1, i, pl.ds(place(k, to), cols), :],
            dst_ref=out.at[:, pl.ds(first_row(k, i), tile)],
            send_sem=half_send.at[k - 1, i, s], recv_sem=half_recv.at[k - 1, i, s],
            device_id=(tp, to), device_id_type=MESH)

    def keep_half(k, i):
        return pltpu.make_async_copy(
            de_half.at[k - 1, i, pl.ds(place(k, me), cols), :],
            out.at[:, pl.ds(first_row(k, i), tile)], half_own.at[k - 1, i])

    begin(0, 0, 0)
    du_ref[...] = jnp.zeros(du_ref.shape, jnp.float32)
    tsum_ref[...] = jnp.zeros(tsum_ref.shape, jnp.float32)
    quarter = dim // 4
    for j in range(2):
        lines = pl.ds(pl.multiple_of(j * wide + x_pos * quarter, 16), quarter)
        ut_half[0, j * quarter:(j + 1) * quarter, :] = ut_ref[lines, :]
    ut_half[1] = ut_ref[pl.ds(pl.multiple_of(y_pos * wide, 16), wide), :]

    def gradient(rows, slot, buf, counted):
        e = emb_buf[slot]
        z = lax.dot_general(u_ref[rows, :], e, NT, preferred_element_type=jnp.float32)
        w = w_ref[rows, :]
        logz = logz_ref[rows, :]
        acc = jnp.zeros((8, LANES), jnp.float32)
        for h in range(per):
            zh = z[:, h * LANES:(h + 1) * LANES]
            q = dense_buf[slot, h, rows, :] * w
            g_buf[buf, rows, h * LANES:(h + 1) * LANES] = (jnp.exp(zh - logz) * w - q).astype(jnp.bfloat16)
            if counted:
                acc = acc + jnp.sum((q * zh).reshape(chunk // 8, 8, LANES), axis=0)
        if counted:
            tsum_ref[...] += acc
            du_ref[rows, :] += jnp.dot(g_buf[buf, rows, :], e, preferred_element_type=jnp.float32)

    def own_step(i, _):
        slot = lax.rem(i, 2)
        arrive(0, i, slot)

        @pl.when(i + 1 < own)
        def _():
            begin(0, i + 1, 1 - slot)

        @pl.when(i + 1 == own)
        def _():
            begin(1, 0, 0)

        def part(c, _):
            gradient(pl.ds(pl.multiple_of(c * chunk, chunk), chunk), slot, 0, True)
            return 0

        lax.fori_loop(0, 2, part, 0)
        de_buf[i] = jnp.dot(ut_ref[...], g_buf[0], preferred_element_type=jnp.float32)
        keep(i).start()
        for s in range(peers - 1, 0, -1):
            send(i, s).start()
        return 0

    lax.fori_loop(0, own, own_step, 0)

    def send_shared(i):
        for k in (1, 2):
            for s in (3, 2, 1):
                send_half(k, i, s).start()

    def store(k, i):
        return pltpu.make_async_copy(g_buf.at[k - 1], g_keep.at[k - 1, i], g_put.at[k - 1])

    def load(k, i):
        return pltpu.make_async_copy(g_keep.at[k - 1, i], g_buf.at[k - 1], g_get.at[k - 1])

    def shared_step(i, _):
        for k, half in ((1, x_pos), (2, y_pos)):
            slot = k - 1
            arrive(k, i, slot)
            if k == 1:
                begin(2, i, 1)
            else:
                @pl.when(i + 1 < shared)
                def _():
                    begin(1, i + 1, 0)
            @pl.when(i > 0)
            def _():
                store(k, i - 1).wait()

            gradient(pl.ds(pl.multiple_of((1 - half) * chunk, chunk), chunk), slot, slot, False)
            gradient(pl.ds(pl.multiple_of(half * chunk, chunk), chunk), slot, slot, True)
            store(k, i).start()
        return 0

    lax.fori_loop(0, shared, shared_step, 0)
    for k in (1, 2):
        store(k, shared - 1).wait()
        load(k, 0).start()

    def late_step(i, _):
        for k in (1, 2):
            load(k, i).wait()
            de_half[k - 1, i] = jnp.dot(ut_half[k - 1], g_buf[k - 1], preferred_element_type=jnp.float32)
            keep_half(k, i).start()

            @pl.when(i + 1 < shared)
            def _():
                load(k, i + 1).start()

        @pl.when(i < shared - held)
        def _():
            send_shared(i)

        return 0

    def to_core(q):
        rows = pl.ds(pl.multiple_of((2 * q + (1 - core)) * local, local), local)
        return pltpu.make_async_remote_copy(
            src_ref=du_ref.at[rows, :], dst_ref=core_buf.at[q], send_sem=red_send.at[q], recv_sem=red_recv.at[q],
            device_id=(tp, me ^ 1), device_id_type=MESH)

    for q in range(pairs):
        to_core(q).start()
    lax.fori_loop(0, 2, late_step, 0)
    for q in range(pairs):
        to_core(q).wait()
    for q in range(pairs):
        core_buf[q] += du_ref[pl.ds(pl.multiple_of((2 * q + core) * local, local), local), :]

    def to_z(s):
        there = tp ^ s
        return pltpu.make_async_remote_copy(
            src_ref=core_buf.at[:, pl.ds(pl.multiple_of(there * part_rows, part_rows), part_rows), :], dst_ref=z_buf.at[s],
            send_sem=red_send.at[pairs + s], recv_sem=red_recv.at[pairs + s],
            device_id=(there, me), device_id_type=MESH)

    for s in range(1, groups):
        to_z(s).start()
    lax.fori_loop(2, shared, late_step, 0)
    for s in range(1, groups):
        to_z(s).wait()
    mine = core_buf[:, pl.ds(pl.multiple_of(tp * part_rows, part_rows), part_rows), :]
    for s in range(1, groups):
        mine += z_buf[s]
    z_buf[0] = mine

    def to_chip(s):
        there = chip ^ s
        return pltpu.make_async_remote_copy(
            src_ref=z_buf.at[0, there], dst_ref=xy_buf.at[s],
            send_sem=red_send.at[pairs + groups + s], recv_sem=red_recv.at[pairs + groups + s],
            device_id=(tp, 2 * there + core), device_id_type=MESH)

    for s in range(1, pairs):
        to_chip(s).start()

    def late(i, _):
        send_shared(i)
        return 0

    lax.fori_loop(shared - held, shared, late, 0)
    for s in range(1, pairs):
        to_chip(s).wait()
    total = z_buf[0, chip]
    for s in range(1, pairs):
        total += xy_buf[s]
    tot_ref[...] = total
    here = pl.ds(pl.multiple_of(tp * part_rows, part_rows), part_rows)
    du_out[here, :] = total

    def share(s):
        return pltpu.make_async_remote_copy(
            src_ref=tot_ref, dst_ref=du_out.at[here, :],
            send_sem=red_send.at[2 * pairs + groups + s], recv_sem=red_recv.at[2 * pairs + groups + s],
            device_id=(tp ^ s, me), device_id_type=MESH)

    for s in range(1, groups):
        share(s).start()

    dw = jnp.sum(total * y_ref[here, :], axis=0, keepdims=True)
    rows = [dw[:, i * 128:(i + 1) * 128] for i in range(dim // 128)]
    rows.append(jnp.sum(tsum_ref[...], axis=0, keepdims=True))
    rows.append(jnp.zeros((16 - len(rows), 128), jnp.float32))
    sums = jnp.concatenate(rows, axis=0)
    mine_ref[...] = sums
    sums_ref[tp * peers + me] = sums
    start, wait = swap_all(mine_ref, sums_ref, all_send, all_recv, groups, peers)
    start()
    for s in range(1, groups):
        share(s).wait()
    du_full[...] = du_out[...]
    wait()
    sums_out[...] = jnp.sum(sums_ref[...], axis=0)

    def drain(i, _):
        keep(i).wait()
        for s in range(1, peers):
            send(i, s).wait()
        return 0

    lax.fori_loop(0, own, drain, 0)

    def drain_half(i, _):
        for k in (1, 2):
            keep_half(k, i).wait()
            for s in (1, 2, 3):
                send_half(k, i, s).wait()
        return 0

    lax.fori_loop(0, shared, drain_half, 0)


def main_pass(emb, dense, u, ut, logz, w, y, own, shared, groups, peers, tile=TILE, held=HELD):
    vocab, dim = emb.shape
    toks = u.shape[0]
    per = tile // LANES
    total = groups * peers
    local = toks // peers
    pairs = peers // 2
    f32 = jnp.float32
    vmem = pl.BlockSpec(memory_space=pltpu.VMEM)
    hbm = pl.BlockSpec(memory_space=pl.ANY)
    red = 2 * pairs + 2 * groups
    return pl.pallas_call(
        functools.partial(main_kernel, tile=tile, own=own, shared=shared, held=held, groups=groups, peers=peers),
        in_specs=[hbm, hbm, vmem, vmem, vmem, vmem, vmem],
        out_specs=[hbm, hbm, vmem, vmem],
        out_shape=[
            jax.ShapeDtypeStruct((dim // peers, vocab), f32),
            jax.ShapeDtypeStruct((2, shared, toks, tile), jnp.bfloat16),
            jax.ShapeDtypeStruct((local, dim), f32),
            jax.ShapeDtypeStruct((16, 128), f32),
        ],
        scratch_shapes=[
            pltpu.VMEM((2, tile, dim), jnp.bfloat16),
            pltpu.VMEM((2, per, toks, LANES), f32),
            pltpu.VMEM((2, toks, tile), jnp.bfloat16),
            pltpu.VMEM((2, dim // 2, toks), jnp.bfloat16),
            pltpu.VMEM((own, dim, tile), f32),
            pltpu.VMEM((2, shared, dim // 2, tile), f32),
            pltpu.VMEM((toks, dim), f32),
            pltpu.VMEM((8, LANES), f32),
            pltpu.VMEM((pairs, local, dim), f32),
            pltpu.VMEM((groups, pairs, local // groups, dim), f32),
            pltpu.VMEM((pairs, local // groups, dim), f32),
            pltpu.VMEM((local // groups, dim), f32),
            pltpu.VMEM((16, 128), f32),
            pltpu.VMEM((local, dim), f32),
            pltpu.VMEM((total, 16, 128), f32),
            pltpu.SemaphoreType.DMA((2, 2)),
            pltpu.SemaphoreType.DMA((2,)),
            pltpu.SemaphoreType.DMA((2,)),
            pltpu.SemaphoreType.DMA((own, peers)),
            pltpu.SemaphoreType.DMA((own, peers)),
            pltpu.SemaphoreType.DMA((own,)),
            pltpu.SemaphoreType.DMA((2, shared, 4)),
            pltpu.SemaphoreType.DMA((2, shared, 4)),
            pltpu.SemaphoreType.DMA((2, shared)),
            pltpu.SemaphoreType.DMA((red,)),
            pltpu.SemaphoreType.DMA((red,)),
            pltpu.SemaphoreType.DMA((total,)),
            pltpu.SemaphoreType.DMA((total,)),
        ],
        compiler_params=pltpu.CompilerParams(vmem_limit_bytes=63 * MIB, collective_id=0, has_side_effects=True),
        cost_estimate=pl.CostEstimate(flops=6 * vocab // peers * dim * toks, bytes_accessed=4 * vocab // peers * toks, transcendentals=vocab // peers * toks),
    )(emb, dense, u, ut, logz, w, y)


def solution(mesh):
    peers = mesh.shape['dp']
    groups = mesh.shape['tp']

    def local_head(hidden, embedding, norm_weight, teach_ids, teach_prob, tok_mask):
        vocab_local = embedding.shape[0]
        toks = hidden.shape[0]
        dim = hidden.shape[1]
        tp = lax.axis_index('tp')
        dp = lax.axis_index('dp')
        scale_w = 1.0 + norm_weight
        h_f32 = hidden.astype(jnp.float32)
        inv_rms = lax.rsqrt(jnp.mean(h_f32 * h_f32, axis=1, keepdims=True) + EPS_NORM)
        normed = h_f32 * inv_rms

        ids_all = lax.all_gather(teach_ids, 'dp', axis=0, tiled=True)
        prob_all = lax.all_gather(teach_prob, 'dp', axis=0, tiled=True)
        normed_all = lax.all_gather(normed, 'dp', axis=0, tiled=True)

        u_loc = (normed * scale_w).astype(jnp.bfloat16)
        stats = local_stats(embedding, u_loc.T, tok_mask.reshape(1, -1), groups, peers)
        stats = stats.reshape(groups, peers, 8, toks)
        row_max = jnp.max(stats[:, :, 0], axis=0)
        sum_exp = jnp.sum(stats[:, :, 1] * jnp.exp(stats[:, :, 0] - row_max), axis=0)
        log_norm = (row_max + jnp.log(sum_exp)).reshape(-1, 1)
        mask = stats[0, :, 2].reshape(-1, 1)
        weight = mask / jnp.sum(mask)

        tiles = vocab_local // TILE
        own = OWN
        shared = tiles // peers - own
        core, chip = dp % 2, dp // 2
        starts = [dp * own, peers * own + (2 * (chip // 2) + core) * shared, peers * own + (peers // 2) * shared + (2 * (chip % 2) + core) * shared]
        base = (jnp.stack(starts) * (TILE // LANES) + tp * (vocab_local // LANES)).astype(jnp.int32)
        regions = tuple(n * (TILE // LANES) for n in (own, shared, shared))
        dense = teacher_dense(base, ids_all, prob_all, regions)
        u_all = (normed_all * scale_w).astype(jnp.bfloat16)
        de_t, _, grad_u, sums = main_pass(embedding, dense, u_all, u_all.T, log_norm, weight, normed, own, shared, groups, peers)
        used = dim // 128
        grad_norm = sums[:used].reshape(dim)
        loss_mean = jnp.sum(weight * log_norm) - jnp.sum(sums[used])
        d_normed = grad_u * scale_w
        grad_hidden = (inv_rms * (d_normed - normed * jnp.mean(d_normed * normed, axis=1, keepdims=True))).astype(jnp.bfloat16)
        return loss_mean, grad_hidden, de_t.T, grad_norm

    return jax.shard_map(local_head, mesh=mesh, in_specs=(P('dp', None), P('tp', None), P(None), P('dp', None), P('dp', None), P('dp')), out_specs=(P(), P('dp', None), P('tp', 'dp'), P(None)), check_vma=False)
```
